256 devices in a mesh: blk: 32 (over y, x, core), vec: 8 (over z).
Axes of the slice: x: 4, y: 4, z: 8, core: 2. Of those that a mesh axis runs over, the one named last changes fastest.
Arguments:
- trial: bfloat16 [64, 64, 16384], P('vec', None, 'blk'), may hold values from -0.005859375 to 0.005859375
- coupling: bfloat16 [32, 6, 512, 512], P('blk'), may hold values from -0.09375 to 0.09375
- partners: int32 [32, 6], P('blk'), may hold values from 0 to 31, as said below
- live: int32 [32], P('blk'), may hold values from 1 to 6, as said below
- diag_block: bfloat16 [16384, 512], P('blk'), may hold values from -0.25 to 0.25
- beta_coupling: bfloat16 [64, 64], replicated, may hold values from -0.75 to 0.75
- hdiag: float32 [64, 16384], P(None, 'blk'), may hold values from 0.5 to 4
Outputs:
- correction: bfloat16 [64, 64, 16384], P('vec', None, 'blk')
- subspace: float32 [64, 64], P(None, 'vec')
The draws below stay inside these ranges and needn't reach their ends.
Inputs may be any that keep to these rules, and one draw needn't show every extreme that they name: `partners`: each row holds 6 different block numbers, none equal to the row's own block. `live`: some block uses all 6 slots in every draw.
All inputs are finite; a program needn't handle non-finite values.
Results may differ from the reference program's by a relative error of at most 0.0012.
Values may be sent and summed in bfloat16 or wider, within the bound.
No kernel may reach another device: no remote copies, remote signals or barrier semaphores. Data moves between devices by JAX's collectives and lax.ppermute only.
A program may use at most 128 MiB of HBM per device.

```python
import jax
import jax.numpy as jnp
from jax import lax

K = 64
A_BLK = 512
NBETA = 64
COUP = 6
NBLOCKS = 32
NA = 16384


def draw_partners(key, part):
    nblocks = NA // A_BLK
    keys = jax.random.split(jax.random.fold_in(key, 11), nblocks)

    def one_row(row_key, position):
        order = jax.random.permutation(row_key, nblocks - 1)[:COUP]
        return ((position + 1 + order) % nblocks).astype(jnp.int32)
    return jax.vmap(one_row)(keys, jnp.arange(nblocks, dtype=jnp.int32))


def draw_live(key, part):
    nblocks = NA // A_BLK
    counts = jax.random.randint(jax.random.fold_in(key, 23), (nblocks,), 1, COUP + 1)
    chosen = jax.random.randint(jax.random.fold_in(key, 29), (), 0, nblocks)
    return jnp.where(jnp.arange(nblocks, dtype=jnp.int32) == chosen, COUP, counts).astype(jnp.int32)


def levels(key, shape, shards, least, largest):
    factor_of, own = 1.0, jax.random.fold_in(key, 6)
    for dim, shards_of in shards:
        heights = jnp.exp(jax.random.uniform(jax.random.fold_in(own, dim), (shards_of,), jnp.float32, least / len(shards), largest / len(shards)))
        factor_of = factor_of * jnp.repeat(heights, shape[dim] // shards_of).reshape([-1 if axis == dim else 1 for axis in range(len(shape))])
    return factor_of


def centred(rng, shape, width, bound, pieces=(), kind=jnp.bfloat16):
    result = jax.random.normal(rng, shape, jnp.float32) * width
    if len(pieces) > 0:
        result = levels(rng, shape, pieces, -0.22, 0.18) * result
    return jnp.clip(result, min=-bound, max=bound).astype(kind)


def setup_inputs(seed: int = 0) -> dict:
    splits = jax.random.split(jax.random.key(seed), 8)
    trial = centred(splits[0], (K, NBETA, NA), (1.0 / (NA * NBETA) ** 0.5), 0.005859375, ((0, 8), (2, 32)))
    coupling = centred(splits[1], (NBLOCKS, COUP, A_BLK, A_BLK), (A_BLK * (COUP + 2)) ** -0.5, 0.09375, ((0, 32),))
    partners = draw_partners(jax.random.fold_in(splits[7], 71), 0)
    live = draw_live(jax.random.fold_in(splits[7], 71), 0)
    diag_block = centred(splits[4], (NA, A_BLK), A_BLK ** -0.5, 0.25, ((0, 32),))
    beta_coupling = centred(splits[5], (NBETA, NBETA), NBETA ** -0.5, 0.75)
    hdiag = jnp.clip(0.5 + 3.5 * jax.random.uniform(splits[6], (NBETA, NA), jnp.float32) ** levels(splits[6], (NBETA, NA), ((1, 32),), -0.2, 0.2), 0.5, 4.0)
    return dict(trial=trial, coupling=coupling, partners=partners, live=live, diag_block=diag_block, beta_coupling=beta_coupling, hdiag=hdiag)


def reference(trial, coupling, partners, live, diag_block, beta_coupling, hdiag):
    nblocks = NA // A_BLK
    row_count = K * NBETA
    flat = trial.reshape(row_count, NA)
    diag_three = diag_block.reshape(nblocks, A_BLK, A_BLK)
    contract = (((1,), (1,)), ((), ()))

    def one_block(entries):
        blocks, partner_ids, live_count, own_block, position = entries
        own_rows = lax.dynamic_slice_in_dim(flat, position * A_BLK, A_BLK, 1)
        running = lax.dot_general(own_rows, own_block, contract, preferred_element_type=jnp.float32)
        for member in range(COUP):
            segment = lax.dynamic_slice_in_dim(flat, (partner_ids[member] * A_BLK).astype(jnp.int32), A_BLK, 1)
            term = lax.dot_general(segment, blocks[member], contract, preferred_element_type=jnp.float32)
            running = running + jnp.where(member < live_count, term, jnp.float32(0.0))
        return running
    stacked = lax.map(one_block, (coupling, partners, live, diag_three, jnp.arange(nblocks, dtype=jnp.int32)))
    alpha_part = jnp.transpose(stacked, (1, 0, 2)).reshape(K, NBETA, NA)
    trial_float = trial.astype(jnp.float32)
    beta_part = jnp.einsum('bc,kca->kba', beta_coupling.astype(jnp.float32), trial_float)
    sigma = alpha_part + beta_part + hdiag[None] * trial_float
    subspace = jnp.einsum('kba,lba->kl', trial_float, sigma, precision=lax.Precision.HIGHEST)
    theta = jnp.diagonal(subspace)
    resid = sigma - theta[:, None, None] * trial_float
    gap = theta[:, None, None] - hdiag[None]
    raw = resid * gap / (gap * gap + 0.25)
    msq = lax.optimization_barrier(jnp.mean(raw * raw, axis=(1, 2)))
    correction = (raw * lax.rsqrt(msq + 1e-06)[:, None, None]).astype(jnp.bfloat16)
    return (correction, subspace)
```

```python
import jax
import jax.numpy as jnp
from jax import lax
from jax.experimental import pallas as pl
from jax.experimental.pallas import tpu as pltpu
from jax.sharding import Mesh, PartitionSpec as P

NT = (((1,), (1,)), ((), ()))
NN = (((1,), (0,)), ((), ()))
F32 = jnp.float32


def shift(n, d):
    return [(i, (i + d) % n) for i in range(n)]


def move(a, axis, d):
    return lax.ppermute(a, axis, shift(lax.axis_size(axis), d))


def swap(a):
    return lax.ppermute(a, "core", [(0, 1), (1, 0)])


def spread(unit, first, second):
    right = move(unit, first, 1)
    left = move(unit, first, -1)
    far_r = move(right[0], first, 1)
    far_l = move(left[1], first, -1)
    row = jnp.stack([unit, right, left, jnp.stack([far_r, far_l])])
    up = move(row, second, 1)
    down = move(row, second, -1)
    far_u = move(up[:2], second, 1)
    far_d = move(down[2:], second, -1)
    whole = jnp.stack([row, up, down, jnp.concatenate([far_u, far_d])])
    return whole.reshape(32, *unit.shape[1:])


def place(d):
    return jnp.where(d == 0, 0, jnp.where(d == 3, 1, jnp.where(d == 1, 2, 3)))


def local_kernel(own, diag0, diag1, beta, h0, h1, acc):
    for s, diag, h in ((0, diag0, h0), (1, diag1, h1)):
        x = own[s]
        total = lax.dot_general(x, diag[...], NT, preferred_element_type=F32)
        for k in range(4):
            rows = slice(64 * k, 64 * k + 64)
            part = lax.dot_general(beta[...], x[rows], NN, preferred_element_type=F32)
            acc[s, rows, :] = total[rows] + part + h[...] * x[rows].astype(F32)


def couple_kernel(idx, live, ga, gb, c0, c1, own, acc, out, theta):
    for s, cp in ((0, c0), (1, c1)):
        out[s] = acc[s]

        def body(c, carry, s=s, cp=cp):
            x = jnp.concatenate([ga[idx[0, 6 * s + c]], gb[idx[1, 6 * s + c]]], axis=0)
            out[s] += lax.dot_general(x, cp[c], NT, preferred_element_type=F32)
            return carry

        lax.fori_loop(0, live[s], body, 0)
    for k in range(4):
        rows = slice(64 * k, 64 * k + 64)
        t = sum(jnp.sum(out[s, rows, :] * own[s, rows, :].astype(F32), axis=0, keepdims=True) for s in range(2))
        theta[k : k + 1, :] = jnp.broadcast_to(jnp.sum(t, axis=1, keepdims=True), (1, 128))


def local(trial, coupling, partners, live, diag_block, beta_coupling, hdiag):
    roots, betas, width = trial.shape
    half = roots // 2
    core, x, y, z = (lax.axis_index(n) for n in ("core", "x", "y", "vec"))
    mine = lax.dynamic_slice_in_dim(trial, core * half, half, 0)
    theirs = lax.dynamic_slice_in_dim(trial, (1 - core) * half, half, 0)
    other = swap(theirs)
    own = jnp.stack([mine, other]).reshape(2, half * betas, width)
    coupling = coupling[0]
    coupling_o = swap(coupling)
    diag_o = swap(diag_block)
    hdiag_o = swap(hdiag)
    table = jnp.concatenate([partners[0], live])
    table = jnp.stack([table, swap(table)])
    lives = table[:, 6]
    j = table[:, :6].reshape(-1)
    slot = jnp.where(j % 2 == core, 0, 1)
    px = place((j // 2 % 4 - x) % 4)
    py = place((j // 8 - y) % 4)
    idx = jnp.stack([(py * 4 + px) * 2 + slot, (px * 4 + py) * 2 + slot])

    rows = half * betas // 2
    ga = spread(own[:, :rows], "x", "y")
    gb = spread(own[:, rows:], "y", "x")

    right = left = trial
    ring = [trial]
    for step in range(4):
        right = move(right, "vec", 1)
        ring.append(right)
        if step < 3:
            left = move(left, "vec", -1)
            ring.append(left)
    offsets = (0, 1, 7, 2, 6, 3, 5, 4)

    vmem = pl.BlockSpec(memory_space=pltpu.VMEM)
    smem = pl.BlockSpec(memory_space=pltpu.SMEM)
    acc = pl.pallas_call(
        local_kernel,
        out_shape=jax.ShapeDtypeStruct((2, half * betas, width), F32),
        in_specs=[vmem] * 6,
        out_specs=vmem,
        cost_estimate=pl.CostEstimate(flops=2 * 512 * 512 * 600, bytes_accessed=4 << 20, transcendentals=0),
        name="local_part",
    )(own, diag_block, diag_o, beta_coupling, hdiag, hdiag_o)
    sigma, theta_part = pl.pallas_call(
        couple_kernel,
        out_shape=(
            jax.ShapeDtypeStruct((2, half * betas, width), F32),
            jax.ShapeDtypeStruct((half, 128), F32),
        ),
        in_specs=[smem] * 2 + [vmem] * 6,
        out_specs=(vmem, vmem),
        cost_estimate=pl.CostEstimate(flops=2 * 512 * 512 * 256 * 12, bytes_accessed=16 << 20, transcendentals=0),
        name="couple_part",
    )(idx, lives, ga, gb, coupling, coupling_o, own, acc)

    everyone = ("y", "x", "core")
    blocks = lax.axis_size("y") * lax.axis_size("x") * 2
    sigma_o = swap(sigma[1])
    chips = blocks // 2
    theta = lax.all_to_all(jnp.broadcast_to(theta_part[None, :, :1].reshape(1, 1, half), (chips, 1, half)), ("y", "x"), 0, 0, tiled=True)
    theta = jnp.sum(theta, axis=(0, 1))[None, :, None, None]

    sig4 = sigma.reshape(2, half, betas, width)
    own4 = own.reshape(2, half, betas, width).astype(F32)
    gap = theta - jnp.stack([hdiag, hdiag_o])[:, None]
    raw = (sig4 - theta * own4) * gap / (gap * gap + 0.25)
    raw_o = swap(raw[1])
    square = jnp.sum(raw * raw, axis=(0, 2, 3))

    sig_other = sigma_o.reshape(half, betas, width)
    first = jnp.where(core == 0, sig4[0], sig_other)
    second = jnp.where(core == 0, sig_other, sig4[0])
    sig_all = jnp.concatenate([first, second])
    hi = sig_all.astype(jnp.bfloat16)
    rest = sig_all - hi.astype(F32)
    mid = rest.astype(jnp.bfloat16)
    low = (rest - mid.astype(F32)).astype(jnp.bfloat16)
    pieces = jnp.concatenate([hi, mid, low])
    all_roots = jnp.concatenate(ring)
    sub = jnp.einsum("kba,lba->kl", all_roots, pieces, preferred_element_type=F32)
    sub = jnp.sum(sub.reshape(8, roots, 3, roots), axis=2)
    source = (z - jnp.array(offsets)) % 8
    pick = (jnp.arange(8)[:, None] == source[None, :]).astype(F32)
    sub = jnp.sum(pick[:, :, None, None] * sub[None], axis=1)

    eight = jnp.where(jnp.arange(roots) // half == core, jnp.tile(square, 2), 0.0)
    packed = jnp.concatenate([eight, sub.reshape(-1)])
    total = lax.all_to_all(jnp.broadcast_to(packed[None, None], (blocks, 1, packed.size)), everyone, 0, 0, tiled=True)
    total = jnp.sum(total, axis=(0, 1))
    scale = lax.rsqrt(total[:roots] / (betas * width * blocks) + 1e-06)
    low_raw = jnp.where(core == 0, raw[0], raw_o)
    high_raw = jnp.where(core == 0, raw_o, raw[0])
    correction = (jnp.concatenate([low_raw, high_raw]) * scale[:, None, None]).astype(jnp.bfloat16)
    return correction, total[roots:].reshape(8 * roots, roots)


def solution(mesh):
    blocks, vecs = mesh.devices.shape
    fine = Mesh(mesh.devices.reshape(4, 4, 2, vecs), ("y", "x", "core", "vec"))
    blk = ("y", "x", "core")
    in_specs = (
        P("vec", None, blk),
        P(blk, None, None, None),
        P(blk, None),
        P(blk),
        P(blk, None),
        P(),
        P(None, blk),
    )
    out_specs = (P("vec", None, blk), P(None, "vec"))
    return jax.shard_map(local, mesh=fine, in_specs=in_specs, out_specs=out_specs, check_vma=False)
```
